32 devices in a mesh: dp: 16 (over z, y, x), mp: 2 (over core).
Axes of the slice: x: 2, y: 2, z: 4, core: 2. Of those that a mesh axis runs over, the one named last changes fastest.
Arguments:
- normed: bfloat16 [6144, 2048], P(('dp', 'mp')), may hold values from -12 to 12
- key_grad: bfloat16 [6144, 512], P('dp', 'mp'), may hold values from -0.078125 to 0.078125
- stale: bfloat16 [16, 2048, 512], P('dp', None, 'mp'), may hold values from -1.5 to 1.5
- worker_flag: int32 [16], P('dp'), may hold values 0 or 1
- block_mask: int32 [16, 4], P('dp'), may hold values 0 or 1
- aggregate: float32 [2048, 512], P('dp', 'mp'), may hold values from -6 to 6
- master: float32 [2048, 512], P('dp', 'mp'), may hold values from -0.125 to 0.125
- moment_one: float32 [2048, 512], P('dp', 'mp'), may hold values from -6 to 6
- moment_two: float32 [2048, 512], P('dp', 'mp'), may hold values from 0.5 to 4
Outputs:
- new_aggregate: float32 [2048, 512], P('dp', 'mp')
- new_master: float32 [2048, 512], P('dp', 'mp')
- new_moment_one: float32 [2048, 512], P('dp', 'mp')
- new_moment_two: float32 [2048, 512], P('dp', 'mp')
- weights: bfloat16 [2048, 512], P(None, 'mp')
- new_stale: bfloat16 [16, 2048, 512], P('dp', None, 'mp')
The draws below stay inside these ranges and needn't reach their ends.
All inputs are finite; a program needn't handle non-finite values. No bound on the sum of `worker_flag` on one device may be relied on, other than what follows from the above.
Results may differ from the reference program's by a relative error of at most 0.0004.
Values may be sent and summed in bfloat16 or wider, within the bound.
A program may use at most 64 MiB of HBM per device.

```python
import math
import jax
import jax.numpy as jnp
from jax import lax

D = 2048
H = 512
BLOCKS = 4
STEP = 10
TOK_DEV = 384
TOKENS = 6144
N_DP = 16


def place_ends(values, key, least, largest):
    extent = values.shape
    index_at = [jax.random.randint(jax.random.fold_in(key, axis), (), 0, extent[axis]) for axis in range(len(extent))]
    values = values.at[tuple(index_at)].set(least)
    longest = extent.index(max(extent))
    index_at[longest] = (index_at[longest] + 1) % extent[longest]
    return values.at[tuple(index_at)].set(largest)


def with_spikes(array, own_key, source, target, blocks, factor):
    def block_of(dim):
        return (jnp.arange(array.shape[dim]) // (array.shape[dim] // blocks)).reshape((-1,) + (1,) * (array.ndim - 1 - dim))

    near = jax.random.permutation(own_key, blocks)[block_of(target)]
    far = (block_of(target) + blocks // 2) % blocks
    return jnp.where((block_of(source) == near) | (block_of(source) == far), factor * array, array)


def block_scale(rng, dims, split, smallest, high):
    level, own = 1.0, jax.random.fold_in(rng, 6)
    for dim, parts in split:
        draws = jnp.exp(jax.random.uniform(jax.random.fold_in(own, dim), (parts,), jnp.float32, smallest / len(split), high / len(split)))
        level = level * jnp.repeat(draws, dims[dim] // parts).reshape([-1 if axis == dim else 1 for axis in range(len(dims))])
    return level


def normal_values(stream_key, extent, width, bound, shards=(), held_as=jnp.bfloat16):
    loudness = block_scale(stream_key, extent, shards, -0.22, 0.18) if shards else 1.0
    drawn = jax.random.normal(stream_key, extent, jnp.float32) * width * loudness
    return jnp.minimum(jnp.maximum(drawn, -bound), bound).astype(held_as)


def bell_draw_with(rng, shape, spread, most, cuts, heavy, kind=jnp.bfloat16):
    entries = spread * jax.random.normal(rng, shape, jnp.float32)
    if cuts:
        entries = entries * block_scale(rng, shape, cuts, -0.22, 0.18)
    return jnp.clip(with_spikes(entries, jax.random.fold_in(rng, 3), *heavy), -most, most).astype(kind)


def setup_inputs(seed: int = 0) -> dict:
    streams_of = jax.random.split(jax.random.key(seed), 10)
    return {
        "normed": bell_draw_with(streams_of[0], (TOKENS, D), 1.0, 12.0, ((0, 32),), (0, 1, 32, 2.75)),
        "key_grad": normal_values(streams_of[1], (TOKENS, H), ((TOK_DEV * N_DP) ** -0.5), 0.078125, ((0, 16), (1, 2))),
        "stale": normal_values(streams_of[2], (N_DP, D, H), (N_DP ** -0.5), 1.5, ((0, 16), (2, 2))),
        "worker_flag": place_ends((jax.random.randint(streams_of[3], (N_DP,), 0, 2) < 1).astype(jnp.int32), jax.random.fold_in(streams_of[3], 1), 0, 1),
        "block_mask": place_ends((jax.random.randint(streams_of[4], (N_DP, BLOCKS), 0, 3) < 2).astype(jnp.int32), jax.random.fold_in(streams_of[4], 1), 0, 1),
        "aggregate": normal_values(streams_of[5], (D, H), 1.0, 6.0, ((0, 16), (1, 2)), jnp.float32),
        "master": normal_values(streams_of[6], (D, H), 0.02, 0.125, ((0, 16), (1, 2)), jnp.float32),
        "moment_one": normal_values(streams_of[7], (D, H), 1.0, 6.0, ((0, 16), (1, 2)), jnp.float32),
        "moment_two": jnp.clip(jnp.exp(math.log(4.0) - 2.0794415 * jax.random.uniform(streams_of[8], (D, H), jnp.float32) ** block_scale(streams_of[8], (D, H), ((0, 16), (1, 2)), -0.2, 0.2)), 0.5, 4.0),
    }


beta_one = 0.9
beta_two = 0.95
learn_rate = 0.001
decay_rate = 0.1
epsilon = 1e-08

def reference(normed, key_grad, stale, worker_flag, block_mask, aggregate, master, moment_one, moment_two):
    column_block = jnp.arange(H, dtype=jnp.int32) // (H // BLOCKS)
    onehot = (column_block[:, None] == jnp.arange(BLOCKS, dtype=jnp.int32)[None, :]).astype(jnp.int32)
    per_column = lax.optimization_barrier(jnp.sum(block_mask[:, None, :] * onehot[None, :, :], axis=2))
    trig_all = worker_flag[:, None] * per_column
    in_rows = normed.reshape(N_DP, TOK_DEV, D)
    out_rows = key_grad.reshape(N_DP, TOK_DEV, H)

    def one_worker(total, items):
        inputs, grad_out, old, trig = items
        grad = lax.dot_general(inputs, grad_out, (((0,), (0,)), ((), ())), preferred_element_type=jnp.float32)
        weight = trig.astype(jnp.float32)
        total = total + weight[None, :] * (grad - old.astype(jnp.float32))
        kept = jnp.where(trig[None, :] > 0, grad.astype(jnp.bfloat16), old)
        return (total, kept)
    summed, new_stale = lax.scan(one_worker, jnp.zeros((D, H), jnp.float32), (in_rows, out_rows, stale, trig_all))
    new_aggregate = aggregate + summed
    grads = new_aggregate
    new_moment_one = beta_one * moment_one + (1.0 - beta_one) * grads
    new_moment_two = beta_two * moment_two + (1.0 - beta_two) * grads * grads
    first_hat = new_moment_one / (1.0 - beta_one ** STEP)
    second_hat = new_moment_two / (1.0 - beta_two ** STEP)
    update = first_hat / (jnp.sqrt(second_hat) + epsilon)
    new_master = master - learn_rate * (update + decay_rate * master)
    weights = new_master.astype(jnp.bfloat16)
    return (new_aggregate, new_master, new_moment_one, new_moment_two, weights, new_stale)
```

```python
import functools
import math

import jax
import jax.numpy as jnp
from jax import lax
from jax.experimental import pallas as pl
from jax.experimental.pallas import tpu as pltpu
from jax.sharding import PartitionSpec as P

H = 512
BLOCKS = 4
STEP = 10


beta_one = 0.9
beta_two = 0.95
learn_rate = 0.001
decay_rate = 0.1
epsilon = 1e-08

LANES = 128
WIRE = jnp.float32
MESH = pl.DeviceIdType.MESH


def grid_of(workers):
    inner = max(i for i in range(1, math.isqrt(workers // 2) + 1) if workers % (i * i) == 0)
    return workers // (inner * inner), inner


def encode(values):
    return values


def decode(values):
    return values


def kernel(
    zs, ins, mps, width,
    normed, key_grad, stale, flag, mask, aggregate, master, moment_one, moment_two,
    out_aggregate, out_master, out_one, out_two, out_weights, out_stale,
    mine, theirs, kgrad, old, kept, states,
    part, wire, got_one, sum_one, wire_two, got_two, wire_three, own_sum, got_three,
    load_sem, store_sem, mp_send, mp_recv, one_send, one_recv, two_send, two_recv,
    three_send, three_recv, gz_send, gz_recv, gs_send, gs_recv, gl_send, gl_recv,
):
    me = lax.axis_index("dp")
    core = lax.axis_index("mp")
    z, a, b = me // (ins * ins), lax.rem(me // ins, ins), lax.rem(me, ins)
    tokens = normed.shape[0]
    slab = normed.shape[1] // zs
    rows = slab // (ins * ins)
    cols = key_grad.shape[1]

    def at(zz, aa, bb):
        return {"dp": (zz * ins + aa) * ins + bb}

    def hop(base, j, size):
        return lax.rem(base + j, size)

    loads = [
        pltpu.make_async_copy(src, dst, load_sem.at[i])
        for i, (src, dst) in enumerate(
            [(normed, mine), (key_grad, kgrad), (stale.at[0], old)]
            + [(src, states.at[i]) for i, src in enumerate((aggregate, master, moment_one, moment_two))]
        )
    ]
    for load in loads:
        load.start()

    peers = [{"mp": hop(core, j, mps)} for j in range(1, mps)]
    peers += [at(hop(z, j, zs), a, b) for j in range(1, zs)]
    peers += [at(z, hop(a, j, ins), b) for j in range(1, ins)]
    peers += [at(z, a, hop(b, j, ins)) for j in range(1, ins)]
    barrier = pltpu.get_barrier_semaphore()
    for peer in peers:
        pl.semaphore_signal(barrier, inc=1, device_id=peer, device_id_type=MESH)
    pl.semaphore_wait(barrier, len(peers))

    pending = []

    def send(src, dst, send_sem, recv_sem, peer):
        copy = pltpu.make_async_remote_copy(
            src_ref=src, dst_ref=dst, send_sem=send_sem, recv_sem=recv_sem,
            device_id=peer, device_id_type=MESH,
        )
        copy.start()
        pending.append(copy)
        return copy

    order = list(range(1, zs)) + [0]
    shared = {}
    for k in order:
        columns = pl.ds(pl.multiple_of(hop(z, k, zs) * slab, slab), slab)
        shared[k] = [
            send(
                normed.at[:, columns], theirs.at[j - 1, :, columns],
                mp_send.at[k, j - 1], mp_recv.at[k, j - 1], {"mp": hop(core, j, mps)},
            )
            for j in range(1, mps)
        ]

    block = (core * cols + lax.broadcasted_iota(jnp.int32, (1, cols), 1)) // width
    trig = jnp.zeros((1, cols), jnp.int32)
    for i in range(BLOCKS):
        trig = trig + jnp.where(block == i, flag[0] * mask[0, i], 0)
    weight = trig.astype(jnp.float32)

    for load in loads[:3]:
        load.wait()

    stores = []

    def compute(k):
        base = pl.multiple_of(hop(z, k, zs) * slab, slab)
        columns = pl.ds(base, slab)

        def product(left, owner):
            held = kgrad[pl.ds(pl.multiple_of(owner * tokens, tokens), tokens), :]
            return lax.dot_general(
                left, held, (((0,), (0,)), ((), ())), preferred_element_type=jnp.float32
            )

        grad = product(mine[:, columns], core)
        for j in range(1, mps):
            shared[k][j - 1].wait_recv()
            grad = grad + product(theirs[j - 1, :, columns], hop(core, mps - j, mps))
        before = old[pl.ds(base, slab), :].astype(jnp.float32)
        kept[pl.ds(base, slab), :] = jnp.where(trig > 0, grad, before).astype(jnp.bfloat16)
        change = weight * (grad - before)
        for s in range(2):
            piece = change[:, s * LANES:(s + 1) * LANES].reshape(ins, ins, rows, LANES)
            part[s, k] = piece
            if WIRE != jnp.float32:
                wire[s, k] = encode(piece)
        store = pltpu.make_async_copy(
            kept.at[pl.ds(base, slab), :], out_stale.at[0, pl.ds(base, slab), :], store_sem.at[k]
        )
        store.start()
        stores.append(store)

    firsts, seconds, thirds = {}, {}, {}
    source = part if WIRE == jnp.float32 else wire
    source_two = sum_one if WIRE == jnp.float32 else wire_two

    def send_one(k):
        firsts[k] = []
        for j in range(1, ins):
            bb, aa = hop(b, j, ins), hop(a, j, ins)
            firsts[k].append((
                send(source.at[0, k, :, bb], got_one.at[0, k, j - 1],
                     one_send.at[0, k, j - 1], one_recv.at[0, k, j - 1], at(z, a, bb)),
                send(source.at[1, k, aa], got_one.at[1, k, j - 1],
                     one_send.at[1, k, j - 1], one_recv.at[1, k, j - 1], at(z, aa, b)),
            ))

    def send_two(k):
        for s in range(2):
            total = part[0, k, :, b] if s == 0 else part[1, k, a]
            for j in range(1, ins):
                firsts[k][j - 1][s].wait_recv()
                total = total + decode(got_one[s, k, j - 1])
            sum_one[s, k] = total
            if WIRE != jnp.float32:
                wire_two[s, k] = encode(total)
        seconds[k] = []
        for j in range(1, ins):
            bb, aa = hop(b, j, ins), hop(a, j, ins)
            seconds[k].append((
                send(source_two.at[0, k, aa], got_two.at[0, k, j - 1],
                     two_send.at[0, k, j - 1], two_recv.at[0, k, j - 1], at(z, aa, b)),
                send(source_two.at[1, k, bb], got_two.at[1, k, j - 1],
                     two_send.at[1, k, j - 1], two_recv.at[1, k, j - 1], at(z, a, bb)),
            ))

    def send_three(k):
        for s in range(2):
            total = sum_one[s, k, a if s == 0 else b]
            for j in range(1, ins):
                seconds[k][j - 1][s].wait_recv()
                total = total + decode(got_two[s, k, j - 1])
            if k == 0:
                own_sum[s] = total
            else:
                wire_three[k - 1, s] = encode(total)
        if k:
            thirds[k] = send(wire_three.at[k - 1], got_three.at[k - 1],
                             three_send.at[k - 1], three_recv.at[k - 1], at(hop(z, k, zs), a, b))

    compute(order[0])
    send_one(order[0])
    for i in range(1, zs + 2):
        if i < zs:
            compute(order[i])
            send_one(order[i])
        if 0 <= i - 1 < zs:
            send_two(order[i - 1])
        if 0 <= i - 2 < zs:
            send_three(order[i - 2])

    for load in loads[3:]:
        load.wait()
    for k in range(1, zs):
        thirds[k].wait_recv()
    for s in range(2):
        here = pl.ds(s * LANES, LANES)
        total = own_sum[s]
        for k in range(1, zs):
            total = total + decode(got_three[k - 1, s])
        new_aggregate = states[0, :, here] + total
        out_aggregate[:, here] = new_aggregate
        new_one = beta_one * states[2, :, here] + (1.0 - beta_one) * new_aggregate
        new_two = beta_two * states[3, :, here] + (1.0 - beta_two) * new_aggregate * new_aggregate
        out_one[:, here] = new_one
        out_two[:, here] = new_two
        first_hat = new_one / (1.0 - beta_one**STEP)
        second_hat = new_two / (1.0 - beta_two**STEP)
        update = first_hat / (jnp.sqrt(second_hat) + epsilon)
        held = states[1, :, here]
        new_master = held - learn_rate * (update + decay_rate * held)
        out_master[:, here] = new_master
        out_weights[z, a, b, :, here] = new_master.astype(jnp.bfloat16)

    halves = [pl.ds(s * LANES, LANES) for s in range(2)]
    spread = {
        k: send(out_weights.at[z, a, b], out_weights.at[z, a, b],
                gz_send.at[k - 1], gz_recv.at[k - 1], at(hop(z, k, zs), a, b))
        for k in range(1, zs)
    }
    shorts, longs = {}, {}

    def gather_short(k):
        zz = hop(z, zs - k, zs)
        if k:
            spread[k].wait_recv()
        shorts[k] = []
        for j in range(1, ins):
            bb, aa = hop(b, j, ins), hop(a, j, ins)
            for s, peer in ((0, at(z, aa, b)), (1, at(z, a, bb))):
                ref = out_weights.at[zz, a, b, :, halves[s]]
                shorts[k].append(
                    send(ref, ref, gs_send.at[s, k, j - 1], gs_recv.at[s, k, j - 1], peer)
                )

    def gather_long(k):
        zz = hop(z, zs - k, zs)
        for copy in shorts[k]:
            copy.wait_recv()
        longs[k] = []
        for j in range(1, ins):
            bb, aa = hop(b, j, ins), hop(a, j, ins)
            for s, peer in ((0, at(z, a, bb)), (1, at(z, aa, b))):
                ref = (out_weights.at[zz, :, b, :, halves[0]] if s == 0
                       else out_weights.at[zz, a, :, :, halves[1]])
                longs[k].append(
                    send(ref, ref, gl_send.at[s, k, j - 1], gl_recv.at[s, k, j - 1], peer)
                )

    turn = list(range(zs))
    for i in range(zs + 1):
        if i < zs:
            gather_short(turn[i])
        if i >= 1:
            gather_long(turn[i - 1])
    for k in turn:
        for copy in longs[k]:
            copy.wait_recv()
    for copy in pending:
        copy.wait_send()
    for store in stores:
        store.wait()


def on_device(
    workers, mps,
    normed, key_grad, stale, worker_flag, block_mask, aggregate, master, moment_one, moment_two
):
    zs, ins = grid_of(workers)
    tokens, depth = normed.shape
    cols = key_grad.shape[1]
    rows = aggregate.shape[0]
    f32, bf16 = jnp.float32, jnp.bfloat16
    dma = pltpu.SemaphoreType.DMA
    anywhere = pl.BlockSpec(memory_space=pl.ANY)
    vmem = pl.BlockSpec(memory_space=pltpu.VMEM)
    smem = pl.BlockSpec(memory_space=pltpu.SMEM)
    state = jax.ShapeDtypeStruct((rows, cols), f32)
    one = (2, zs, ins, ins, rows, LANES)
    two = (2, zs, ins, rows, LANES)
    coded = WIRE != f32
    tiny = (1, 1, 1, 1, 8, LANES)
    results = pl.pallas_call(
        functools.partial(kernel, zs, ins, mps, H // BLOCKS),
        out_shape=(
            state, state, state, state,
            jax.ShapeDtypeStruct((zs, ins, ins, rows, cols), bf16),
            jax.ShapeDtypeStruct(stale.shape, bf16),
        ),
        in_specs=[anywhere] * 3 + [smem] * 2 + [anywhere] * 4,
        out_specs=(vmem,) * 5 + (anywhere,),
        scratch_shapes=[
            pltpu.VMEM((tokens, depth), bf16),
            pltpu.VMEM((mps - 1, tokens, depth), bf16),
            pltpu.VMEM(key_grad.shape, bf16),
            pltpu.VMEM((depth, cols), bf16),
            pltpu.VMEM((depth, cols), bf16),
            pltpu.VMEM((4, rows, cols), f32),
            pltpu.VMEM(one, f32),
            pltpu.VMEM(one if coded else tiny, WIRE),
            pltpu.VMEM((2, zs, ins - 1, ins, rows, LANES), WIRE),
            pltpu.VMEM(two, f32),
            pltpu.VMEM(two if coded else tiny[1:], WIRE),
            pltpu.VMEM((2, zs, ins - 1, rows, LANES), WIRE),
            pltpu.VMEM((zs - 1, 2, rows, LANES), WIRE),
            pltpu.VMEM((2, rows, LANES), f32),
            pltpu.VMEM((zs - 1, 2, rows, LANES), WIRE),
            dma((7,)), dma((zs,)),
            dma((zs, mps - 1)), dma((zs, mps - 1)),
            dma((2, zs, ins - 1)), dma((2, zs, ins - 1)),
            dma((2, zs, ins - 1)), dma((2, zs, ins - 1)),
            dma((zs - 1,)), dma((zs - 1,)),
            dma((zs - 1,)), dma((zs - 1,)),
            dma((2, zs, ins - 1)), dma((2, zs, ins - 1)),
            dma((2, zs, ins - 1)), dma((2, zs, ins - 1)),
        ],
        compiler_params=pltpu.CompilerParams(
            collective_id=0, has_side_effects=True, vmem_limit_bytes=48 * 1024 * 1024
        ),
    )(normed, key_grad, stale, worker_flag, block_mask, aggregate, master, moment_one, moment_two)
    return results[:4] + (results[4].reshape(depth, cols), results[5])


def solution(mesh):
    placed = (
        P(("dp", "mp"), None),
        P("dp", "mp"),
        P("dp", None, "mp"),
        P("dp"),
        P("dp", None),
        P("dp", "mp"),
        P("dp", "mp"),
        P("dp", "mp"),
        P("dp", "mp"),
    )
    return jax.shard_map(
        functools.partial(on_device, mesh.shape["dp"], mesh.shape["mp"]),
        mesh=mesh,
        in_specs=placed,
        out_specs=(
            P("dp", "mp"),
            P("dp", "mp"),
            P("dp", "mp"),
            P("dp", "mp"),
            P(None, "mp"),
            P("dp", None, "mp"),
        ),
        check_vma=False,
    )
```

```python
import functools
import math

import jax
import jax.numpy as jnp
from jax import lax
from jax.experimental import pallas as pl
from jax.experimental.pallas import tpu as pltpu
from jax.sharding import PartitionSpec as P

H = 512
BLOCKS = 4
STEP = 10


beta_one = 0.9
beta_two = 0.95
learn_rate = 0.001
decay_rate = 0.1
epsilon = 1e-08

LANES = 128
WIRE = jnp.int16
FINEST = 2.0**14
LEVELS = 1092.0
MESH = pl.DeviceIdType.MESH


def grid_of(workers):
    inner = max(i for i in range(1, math.isqrt(workers // 2) + 1) if workers % (i * i) == 0)
    return workers // (inner * inner), inner


def encode(values):
    size = jnp.log2(1.0 + jnp.abs(values) * FINEST)
    code = jnp.minimum(size * LEVELS + 0.5, 32767.0).astype(jnp.int32)
    return jnp.where(values < 0, -code, code).astype(jnp.int16)


def decode(codes):
    code = codes.astype(jnp.int32).astype(jnp.float32)
    size = (jnp.exp2(jnp.abs(code) * (1.0 / LEVELS)) - 1.0) * (1.0 / FINEST)
    return jnp.where(code < 0, -size, size)


def kernel(
    zs, ins, mps, width,
    normed, key_grad, stale, flag, mask, aggregate, master, moment_one, moment_two,
    out_aggregate, out_master, out_one, out_two, out_weights, kept,
    mine, theirs, kgrad, old, states,
    part, wire, got_one, sum_one, wire_two, got_two, wire_three, own_sum, got_three,
    load_sem, mp_send, mp_recv, one_send, one_recv, two_send, two_recv,
    three_send, three_recv, gz_send, gz_recv, gs_send, gs_recv, gl_send, gl_recv,
):
    me = lax.axis_index("dp")
    core = lax.axis_index("mp")
    z, a, b = me // (ins * ins), lax.rem(me // ins, ins), lax.rem(me, ins)
    tokens = normed.shape[0]
    slab = normed.shape[1] // zs
    rows = slab // (ins * ins)
    cols = key_grad.shape[1]

    def at(zz, aa, bb):
        return {"dp": (zz * ins + aa) * ins + bb}

    def hop(base, j, size):
        return lax.rem(base + j, size)

    loads = [
        pltpu.make_async_copy(src, dst, load_sem.at[i])
        for i, (src, dst) in enumerate(
            [(normed, mine), (key_grad, kgrad), (stale.at[0], old)]
            + [(src, states.at[i]) for i, src in enumerate((aggregate, master, moment_one, moment_two))]
        )
    ]
    for load in loads:
        load.start()

    peers = [{"mp": hop(core, j, mps)} for j in range(1, mps)]
    peers += [at(hop(z, j, zs), a, b) for j in range(1, zs)]
    peers += [at(z, hop(a, j, ins), b) for j in range(1, ins)]
    peers += [at(z, a, hop(b, j, ins)) for j in range(1, ins)]
    barrier = pltpu.get_barrier_semaphore()
    for peer in peers:
        pl.semaphore_signal(barrier, inc=1, device_id=peer, device_id_type=MESH)
    pl.semaphore_wait(barrier, len(peers))

    pending = []

    def send(src, dst, send_sem, recv_sem, peer):
        copy = pltpu.make_async_remote_copy(
            src_ref=src, dst_ref=dst, send_sem=send_sem, recv_sem=recv_sem,
            device_id=peer, device_id_type=MESH,
        )
        copy.start()
        pending.append(copy)
        return copy

    order = list(range(1, zs)) + [0]
    shared = {}
    for k in order:
        columns = pl.ds(pl.multiple_of(hop(z, k, zs) * slab, slab), slab)
        shared[k] = [
            send(
                normed.at[:, columns], theirs.at[j - 1, :, columns],
                mp_send.at[k, j - 1], mp_recv.at[k, j - 1], {"mp": hop(core, j, mps)},
            )
            for j in range(1, mps)
        ]

    block = (core * cols + lax.broadcasted_iota(jnp.int32, (1, cols), 1)) // width
    trig = jnp.zeros((1, cols), jnp.int32)
    for i in range(BLOCKS):
        trig = trig + jnp.where(block == i, flag[0] * mask[0, i], 0)
    weight = trig.astype(jnp.float32)

    for load in loads[:3]:
        load.wait()

    def compute(k):
        base = pl.multiple_of(hop(z, k, zs) * slab, slab)
        columns = pl.ds(base, slab)

        def product(left, owner):
            held = kgrad[pl.ds(pl.multiple_of(owner * tokens, tokens), tokens), :]
            return lax.dot_general(
                left, held, (((0,), (0,)), ((), ())), preferred_element_type=jnp.float32
            )

        grad = product(mine[:, columns], core)
        for j in range(1, mps):
            shared[k][j - 1].wait_recv()
            grad = grad + product(theirs[j - 1, :, columns], hop(core, mps - j, mps))
        before = old[pl.ds(base, slab), :].astype(jnp.float32)
        kept[pl.ds(base, slab), :] = jnp.where(trig > 0, grad, before).astype(jnp.bfloat16)
        change = weight * (grad - before)
        for s in range(2):
            piece = change[:, s * LANES:(s + 1) * LANES].reshape(ins, ins, rows, LANES)
            part[s, k] = piece
            if WIRE != jnp.float32:
                wire[s, k] = encode(piece)

    firsts, seconds, thirds = {}, {}, {}
    source = part if WIRE == jnp.float32 else wire
    source_two = sum_one if WIRE == jnp.float32 else wire_two

    def send_one(k):
        firsts[k] = []
        for j in range(1, ins):
            bb, aa = hop(b, j, ins), hop(a, j, ins)
            firsts[k].append((
                send(source.at[0, k, :, bb], got_one.at[0, k, j - 1],
                     one_send.at[0, k, j - 1], one_recv.at[0, k, j - 1], at(z, a, bb)),
                send(source.at[1, k, aa], got_one.at[1, k, j - 1],
                     one_send.at[1, k, j - 1], one_recv.at[1, k, j - 1], at(z, aa, b)),
            ))

    def send_two(k):
        for s in range(2):
            total = part[0, k, :, b] if s == 0 else part[1, k, a]
            for j in range(1, ins):
                firsts[k][j - 1][s].wait_recv()
                total = total + decode(got_one[s, k, j - 1])
            sum_one[s, k] = total
            if WIRE != jnp.float32:
                wire_two[s, k] = encode(total)
        seconds[k] = []
        for j in range(1, ins):
            bb, aa = hop(b, j, ins), hop(a, j, ins)
            seconds[k].append((
                send(source_two.at[0, k, aa], got_two.at[0, k, j - 1],
                     two_send.at[0, k, j - 1], two_recv.at[0, k, j - 1], at(z, aa, b)),
                send(source_two.at[1, k, bb], got_two.at[1, k, j - 1],
                     two_send.at[1, k, j - 1], two_recv.at[1, k, j - 1], at(z, a, bb)),
            ))

    def send_three(k):
        for s in range(2):
            total = sum_one[s, k, a if s == 0 else b]
            for j in range(1, ins):
                seconds[k][j - 1][s].wait_recv()
                total = total + decode(got_two[s, k, j - 1])
            if k == 0:
                own_sum[s] = total
            else:
                wire_three[k - 1, s] = encode(total)
        if k:
            thirds[k] = send(wire_three.at[k - 1], got_three.at[k - 1],
                             three_send.at[k - 1], three_recv.at[k - 1], at(hop(z, k, zs), a, b))

    compute(order[0])
    send_one(order[0])
    for i in range(1, zs + 2):
        if i < zs:
            compute(order[i])
            send_one(order[i])
        if 0 <= i - 1 < zs:
            send_two(order[i - 1])
        if 0 <= i - 2 < zs:
            send_three(order[i - 2])

    for load in loads[3:]:
        load.wait()
    for k in range(1, zs):
        thirds[k].wait_recv()
    for s in range(2):
        here = pl.ds(s * LANES, LANES)
        total = own_sum[s]
        for k in range(1, zs):
            total = total + decode(got_three[k - 1, s])
        new_aggregate = states[0, :, here] + total
        out_aggregate[:, here] = new_aggregate
        new_one = beta_one * states[2, :, here] + (1.0 - beta_one) * new_aggregate
        new_two = beta_two * states[3, :, here] + (1.0 - beta_two) * new_aggregate * new_aggregate
        out_one[:, here] = new_one
        out_two[:, here] = new_two
        first_hat = new_one / (1.0 - beta_one**STEP)
        second_hat = new_two / (1.0 - beta_two**STEP)
        update = first_hat / (jnp.sqrt(second_hat) + epsilon)
        held = states[1, :, here]
        new_master = held - learn_rate * (update + decay_rate * held)
        out_master[:, here] = new_master
        out_weights[z, a, b, :, here] = new_master.astype(jnp.bfloat16)

    halves = [pl.ds(s * LANES, LANES) for s in range(2)]
    spread = {
        k: send(out_weights.at[z, a, b], out_weights.at[z, a, b],
                gz_send.at[k - 1], gz_recv.at[k - 1], at(hop(z, k, zs), a, b))
        for k in range(1, zs)
    }
    shorts, longs = {}, {}

    def gather_short(k):
        zz = hop(z, zs - k, zs)
        if k:
            spread[k].wait_recv()
        shorts[k] = []
        for j in range(1, ins):
            bb, aa = hop(b, j, ins), hop(a, j, ins)
            for s, peer in ((0, at(z, aa, b)), (1, at(z, a, bb))):
                ref = out_weights.at[zz, a, b, :, halves[s]]
                shorts[k].append(
                    send(ref, ref, gs_send.at[s, k, j - 1], gs_recv.at[s, k, j - 1], peer)
                )

    def gather_long(k):
        zz = hop(z, zs - k, zs)
        for copy in shorts[k]:
            copy.wait_recv()
        longs[k] = []
        for j in range(1, ins):
            bb, aa = hop(b, j, ins), hop(a, j, ins)
            for s, peer in ((0, at(z, a, bb)), (1, at(z, aa, b))):
                ref = (out_weights.at[zz, :, b, :, halves[0]] if s == 0
                       else out_weights.at[zz, a, :, :, halves[1]])
                longs[k].append(
                    send(ref, ref, gl_send.at[s, k, j - 1], gl_recv.at[s, k, j - 1], peer)
                )

    turn = list(range(zs))
    for i in range(zs + 1):
        if i < zs:
            gather_short(turn[i])
        if i >= 1:
            gather_long(turn[i - 1])
    for k in turn:
        for copy in longs[k]:
            copy.wait_recv()
    for copy in pending:
        copy.wait_send()


def write_out(*refs):
    copies = [
        pltpu.make_async_copy(src, dst, refs[12].at[i])
        for i, (src, dst) in enumerate(zip(refs[:6], refs[6:12]))
    ]
    for copy in reversed(copies):
        copy.start()
    for copy in copies:
        copy.wait()


def on_device(
    workers, mps,
    normed, key_grad, stale, worker_flag, block_mask, aggregate, master, moment_one, moment_two
):
    zs, ins = grid_of(workers)
    tokens, depth = normed.shape
    cols = key_grad.shape[1]
    rows = aggregate.shape[0]
    f32, bf16 = jnp.float32, jnp.bfloat16
    dma = pltpu.SemaphoreType.DMA
    hbm = pl.BlockSpec(memory_space=pltpu.HBM)
    vmem = pl.BlockSpec(memory_space=pltpu.VMEM)
    far = functools.partial(pltpu.with_memory_space_constraint, memory_space=pltpu.HBM)
    smem = pl.BlockSpec(memory_space=pltpu.SMEM)
    state = jax.ShapeDtypeStruct((rows, cols), f32)
    one = (2, zs, ins, ins, rows, LANES)
    two = (2, zs, ins, rows, LANES)
    coded = WIRE != f32
    tiny = (1, 1, 1, 1, 8, LANES)
    results = pl.pallas_call(
        functools.partial(kernel, zs, ins, mps, H // BLOCKS),
        out_shape=(
            state, state, state, state,
            jax.ShapeDtypeStruct((zs, ins, ins, rows, cols), bf16),
            jax.ShapeDtypeStruct((depth, cols), bf16),
        ),
        in_specs=[hbm] * 3 + [smem] * 2 + [hbm] * 4,
        out_specs=(vmem,) * 6,
        scratch_shapes=[
            pltpu.VMEM((tokens, depth), bf16),
            pltpu.VMEM((mps - 1, tokens, depth), bf16),
            pltpu.VMEM(key_grad.shape, bf16),
            pltpu.VMEM((depth, cols), bf16),
            pltpu.VMEM((4, rows, cols), f32),
            pltpu.VMEM(one, f32),
            pltpu.VMEM(one if coded else tiny, WIRE),
            pltpu.VMEM((2, zs, ins - 1, ins, rows, LANES), WIRE),
            pltpu.VMEM(two, f32),
            pltpu.VMEM(two if coded else tiny[1:], WIRE),
            pltpu.VMEM((2, zs, ins - 1, rows, LANES), WIRE),
            pltpu.VMEM((zs - 1, 2, rows, LANES), WIRE),
            pltpu.VMEM((2, rows, LANES), f32),
            pltpu.VMEM((zs - 1, 2, rows, LANES), WIRE),
            dma((7,)),
            dma((zs, mps - 1)), dma((zs, mps - 1)),
            dma((2, zs, ins - 1)), dma((2, zs, ins - 1)),
            dma((2, zs, ins - 1)), dma((2, zs, ins - 1)),
            dma((zs - 1,)), dma((zs - 1,)),
            dma((zs - 1,)), dma((zs - 1,)),
            dma((2, zs, ins - 1)), dma((2, zs, ins - 1)),
            dma((2, zs, ins - 1)), dma((2, zs, ins - 1)),
        ],
        compiler_params=pltpu.CompilerParams(
            collective_id=0, has_side_effects=True, vmem_limit_bytes=48 * 1024 * 1024
        ),
    )(
        far(normed), far(key_grad), far(stale), worker_flag, block_mask,
        far(aggregate), far(master), far(moment_one), far(moment_two),
    )
    results = results[:4] + (results[4].reshape(depth, cols), results[5])
    results = pl.pallas_call(
        write_out,
        out_shape=tuple(pltpu.HBM(x.shape, x.dtype) for x in results),
        in_specs=[vmem] * 6,
        out_specs=(hbm,) * 6,
        scratch_shapes=[dma((6,))],
        compiler_params=pltpu.CompilerParams(vmem_limit_bytes=2 * 1024 * 1024),
    )(*results)
    return results[:5] + (results[5][None],)


def solution(mesh):
    placed = (
        P(("dp", "mp"), None),
        P("dp", "mp"),
        P("dp", None, "mp"),
        P("dp"),
        P("dp", None),
        P("dp", "mp"),
        P("dp", "mp"),
        P("dp", "mp"),
        P("dp", "mp"),
    )
    return jax.shard_map(
        functools.partial(on_device, mesh.shape["dp"], mesh.shape["mp"]),
        mesh=mesh,
        in_specs=placed,
        out_specs=(
            P("dp", "mp"),
            P("dp", "mp"),
            P("dp", "mp"),
            P("dp", "mp"),
            P(None, "mp"),
            P("dp", None, "mp"),
        ),
        check_vma=False,
    )
```

```python
import functools
import math

import jax
import jax.numpy as jnp
from jax import lax
from jax.experimental import pallas as pl
from jax.experimental.pallas import tpu as pltpu
from jax.sharding import PartitionSpec as P

H = 512
BLOCKS = 4
STEP = 10


beta_one = 0.9
beta_two = 0.95
learn_rate = 0.001
decay_rate = 0.1
epsilon = 1e-08

LANES = 128
WIRE = jnp.int16
FINEST = 2.0**14
LEVELS = 1092.0
MESH = pl.DeviceIdType.MESH


def grid_of(workers):
    inner = max(i for i in range(1, math.isqrt(workers // 2) + 1) if workers % (i * i) == 0)
    return workers // (inner * inner), inner


def encode(values):
    size = jnp.log2(1.0 + jnp.abs(values) * FINEST)
    code = jnp.minimum(size * LEVELS + 0.5, 32767.0).astype(jnp.int32)
    return jnp.where(values < 0, -code, code).astype(jnp.int16)


def decode(codes):
    code = codes.astype(jnp.int32).astype(jnp.float32)
    size = (jnp.exp2(jnp.abs(code) * (1.0 / LEVELS)) - 1.0) * (1.0 / FINEST)
    return jnp.where(code < 0, -size, size)


def kernel(
    zs, ins, mps, width,
    normed, key_grad, stale, flag, far_mask, aggregate, master, moment_one, moment_two,
    out_aggregate, out_master, out_one, out_two, out_weights, kept,
    mine, theirs, kgrad, old, states,
    part, wire, got_one, sum_one, wire_two, got_two, wire_three, own_sum, got_three,
    mask, load_sem, mp_send, mp_recv, one_send, one_recv, two_send, two_recv,
    three_send, three_recv, gz_send, gz_recv, gs_send, gs_recv, gl_send, gl_recv,
    gd_send, gd_recv,
):
    me = lax.axis_index("dp")
    core = lax.axis_index("mp")
    z, a, b = me // (ins * ins), lax.rem(me // ins, ins), lax.rem(me, ins)
    tokens = normed.shape[0]
    slab = normed.shape[1] // zs
    rows = slab // (ins * ins)
    cols = key_grad.shape[1]

    def at(zz, aa, bb):
        return {"dp": (zz * ins + aa) * ins + bb}

    def hop(base, j, size):
        return lax.rem(base + j, size)

    loads = [
        pltpu.make_async_copy(src, dst, load_sem.at[i])
        for i, (src, dst) in enumerate(
            [(far_mask, mask), (normed, mine), (key_grad, kgrad), (stale.at[0], old)]
            + [(src, states.at[i]) for i, src in enumerate((aggregate, master, moment_one, moment_two))]
        )
    ]
    for load in loads:
        load.start()

    peers = [{"mp": hop(core, j, mps)} for j in range(1, mps)]
    peers += [at(hop(z, j, zs), a, b) for j in range(1, zs)]
    peers += [at(z, hop(a, j, ins), b) for j in range(1, ins)]
    peers += [at(z, a, hop(b, j, ins)) for j in range(1, ins)]
    barrier = pltpu.get_barrier_semaphore()
    for peer in peers:
        pl.semaphore_signal(barrier, inc=1, device_id=peer, device_id_type=MESH)
    pl.semaphore_wait(barrier, len(peers))

    pending = []

    def send(src, dst, send_sem, recv_sem, peer):
        copy = pltpu.make_async_remote_copy(
            src_ref=src, dst_ref=dst, send_sem=send_sem, recv_sem=recv_sem,
            device_id=peer, device_id_type=MESH,
        )
        copy.start()
        pending.append(copy)
        return copy

    order = list(range(1, zs)) + [0]
    shared = {}
    for k in order:
        columns = pl.ds(pl.multiple_of(hop(z, k, zs) * slab, slab), slab)
        shared[k] = [
            send(
                normed.at[:, columns], theirs.at[j - 1, :, columns],
                mp_send.at[k, j - 1], mp_recv.at[k, j - 1], {"mp": hop(core, j, mps)},
            )
            for j in range(1, mps)
        ]

    loads[0].wait()
    block = (core * cols + lax.broadcasted_iota(jnp.int32, (1, cols), 1)) // width
    trig = jnp.zeros((1, cols), jnp.int32)
    for i in range(BLOCKS):
        trig = trig + jnp.where(block == i, flag[0] * mask[0, i], 0)
    weight = trig.astype(jnp.float32)

    for load in loads[1:4]:
        load.wait()

    def compute(k):
        base = pl.multiple_of(hop(z, k, zs) * slab, slab)
        columns = pl.ds(base, slab)

        def product(left, owner):
            held = kgrad[pl.ds(pl.multiple_of(owner * tokens, tokens), tokens), :]
            return lax.dot_general(
                left, held, (((0,), (0,)), ((), ())), preferred_element_type=jnp.float32
            )

        grad = product(mine[:, columns], core)
        for j in range(1, mps):
            shared[k][j - 1].wait_recv()
            grad = grad + product(theirs[j - 1, :, columns], hop(core, mps - j, mps))
        before = old[pl.ds(base, slab), :].astype(jnp.float32)
        kept[pl.ds(base, slab), :] = jnp.where(trig > 0, grad, before).astype(jnp.bfloat16)
        change = weight * (grad - before)
        for s in range(2):
            piece = change[:, s * LANES:(s + 1) * LANES].reshape(ins, ins, rows, LANES)
            part[s, k] = piece

    firsts, seconds, thirds = {}, {}, {}
    source = part if WIRE == jnp.float32 else wire
    source_two = sum_one if WIRE == jnp.float32 else wire_two

    def send_one(k):
        firsts[k] = []
        for j in range(1, ins):
            bb, aa = hop(b, j, ins), hop(a, j, ins)
            if WIRE != jnp.float32:
                wire[0, k, :, bb] = encode(part[0, k, :, bb])
                wire[1, k, aa] = encode(part[1, k, aa])
            firsts[k].append((
                send(source.at[0, k, :, bb], got_one.at[0, k, j - 1],
                     one_send.at[0, k, j - 1], one_recv.at[0, k, j - 1], at(z, a, bb)),
                send(source.at[1, k, aa], got_one.at[1, k, j - 1],
                     one_send.at[1, k, j - 1], one_recv.at[1, k, j - 1], at(z, aa, b)),
            ))

    def send_two(k):
        for s in range(2):
            total = part[0, k, :, b] if s == 0 else part[1, k, a]
            for j in range(1, ins):
                firsts[k][j - 1][s].wait_recv()
                total = total + decode(got_one[s, k, j - 1])
            sum_one[s, k] = total
        seconds[k] = []
        for j in range(1, ins):
            bb, aa = hop(b, j, ins), hop(a, j, ins)
            if WIRE != jnp.float32:
                wire_two[0, k, aa] = encode(sum_one[0, k, aa])
                wire_two[1, k, bb] = encode(sum_one[1, k, bb])
            seconds[k].append((
                send(source_two.at[0, k, aa], got_two.at[0, k, j - 1],
                     two_send.at[0, k, j - 1], two_recv.at[0, k, j - 1], at(z, aa, b)),
                send(source_two.at[1, k, bb], got_two.at[1, k, j - 1],
                     two_send.at[1, k, j - 1], two_recv.at[1, k, j - 1], at(z, a, bb)),
            ))

    def send_three(k):
        for s in range(2):
            total = sum_one[s, k, a if s == 0 else b]
            for j in range(1, ins):
                seconds[k][j - 1][s].wait_recv()
                total = total + decode(got_two[s, k, j - 1])
            if k == 0:
                own_sum[s] = total
            else:
                wire_three[k - 1, s] = encode(total)
        if k:
            thirds[k] = send(wire_three.at[k - 1], got_three.at[k - 1],
                             three_send.at[k - 1], three_recv.at[k - 1], at(hop(z, k, zs), a, b))

    compute(order[0])
    send_one(order[0])
    for i in range(1, zs + 2):
        if i < zs:
            compute(order[i])
            send_one(order[i])
        if 0 <= i - 1 < zs:
            send_two(order[i - 1])
        if 0 <= i - 2 < zs:
            send_three(order[i - 2])

    for load in loads[4:]:
        load.wait()
    for k in range(1, zs):
        thirds[k].wait_recv()
    for s in range(2):
        here = pl.ds(s * LANES, LANES)
        total = own_sum[s]
        for k in range(1, zs):
            total = total + decode(got_three[k - 1, s])
        new_aggregate = states[0, :, here] + total
        out_aggregate[:, here] = new_aggregate
        new_one = beta_one * states[2, :, here] + (1.0 - beta_one) * new_aggregate
        new_two = beta_two * states[3, :, here] + (1.0 - beta_two) * new_aggregate * new_aggregate
        out_one[:, here] = new_one
        out_two[:, here] = new_two
        first_hat = new_one / (1.0 - beta_one**STEP)
        second_hat = new_two / (1.0 - beta_two**STEP)
        update = first_hat / (jnp.sqrt(second_hat) + epsilon)
        held = states[1, :, here]
        new_master = held - learn_rate * (update + decay_rate * held)
        out_master[:, here] = new_master
        out_weights[z, a, b, :, here] = new_master.astype(jnp.bfloat16)

    halves = [pl.ds(s * LANES, LANES) for s in range(2)]
    spread = {
        k: send(out_weights.at[z, a, b], out_weights.at[z, a, b],
                gz_send.at[k - 1], gz_recv.at[k - 1], at(hop(z, k, zs), a, b))
        for k in range(1, zs)
    }
    shorts, longs, directs = {}, {}, {}

    def gather_all(k, zz):
        ref = out_weights.at[zz, a, b]
        directs[k] = [
            send(ref, ref, gd_send.at[k, j - 1], gd_recv.at[k, j - 1],
                 at(z, hop(a, j // ins, ins), hop(b, j % ins, ins)))
            for j in range(1, ins * ins)
        ]

    def gather_short(k):
        zz = hop(z, zs - k, zs)
        if k:
            spread[k].wait_recv()
        shorts[k] = []
        if k >= zs - 2:
            return gather_all(k, zz)
        for j in range(1, ins):
            bb, aa = hop(b, j, ins), hop(a, j, ins)
            for s, peer in ((0, at(z, aa, b)), (1, at(z, a, bb))):
                ref = out_weights.at[zz, a, b, :, halves[s]]
                shorts[k].append(
                    send(ref, ref, gs_send.at[s, k, j - 1], gs_recv.at[s, k, j - 1], peer)
                )

    def gather_long(k):
        zz = hop(z, zs - k, zs)
        for copy in shorts[k]:
            copy.wait_recv()
        longs[k] = []
        if k >= zs - 2:
            return
        for j in range(1, ins):
            bb, aa = hop(b, j, ins), hop(a, j, ins)
            for s, peer in ((0, at(z, a, bb)), (1, at(z, aa, b))):
                ref = (out_weights.at[zz, :, b, :, halves[0]] if s == 0
                       else out_weights.at[zz, a, :, :, halves[1]])
                longs[k].append(
                    send(ref, ref, gl_send.at[s, k, j - 1], gl_recv.at[s, k, j - 1], peer)
                )

    turn = list(range(zs))
    for i in range(zs + 1):
        if i < zs:
            gather_short(turn[i])
        if i >= 1:
            gather_long(turn[i - 1])
    for k in turn:
        for copy in longs[k] + directs.get(k, []):
            copy.wait_recv()
    for copy in pending:
        copy.wait_send()


def write_out(*refs):
    copies = [
        pltpu.make_async_copy(src, dst, refs[12].at[i])
        for i, (src, dst) in enumerate(zip(refs[:6], refs[6:12]))
    ]
    for copy in reversed(copies):
        copy.start()
    for copy in copies:
        copy.wait()


def on_device(
    workers, mps,
    normed, key_grad, stale, worker_flag, block_mask, aggregate, master, moment_one, moment_two
):
    zs, ins = grid_of(workers)
    tokens, depth = normed.shape
    cols = key_grad.shape[1]
    rows = aggregate.shape[0]
    f32, bf16 = jnp.float32, jnp.bfloat16
    dma = pltpu.SemaphoreType.DMA
    hbm = pl.BlockSpec(memory_space=pltpu.HBM)
    vmem = pl.BlockSpec(memory_space=pltpu.VMEM)
    far = functools.partial(pltpu.with_memory_space_constraint, memory_space=pltpu.HBM)
    smem = pl.BlockSpec(memory_space=pltpu.SMEM)
    state = jax.ShapeDtypeStruct((rows, cols), f32)
    one = (2, zs, ins, ins, rows, LANES)
    two = (2, zs, ins, rows, LANES)
    coded = WIRE != f32
    tiny = (1, 1, 1, 1, 8, LANES)
    results = pl.pallas_call(
        functools.partial(kernel, zs, ins, mps, H // BLOCKS),
        out_shape=(
            state, state, state, state,
            jax.ShapeDtypeStruct((zs, ins, ins, rows, cols), bf16),
            jax.ShapeDtypeStruct((depth, cols), bf16),
        ),
        in_specs=[hbm] * 3 + [smem] + [hbm] * 5,
        out_specs=(vmem,) * 6,
        scratch_shapes=[
            pltpu.VMEM((tokens, depth), bf16),
            pltpu.VMEM((mps - 1, tokens, depth), bf16),
            pltpu.VMEM(key_grad.shape, bf16),
            pltpu.VMEM((depth, cols), bf16),
            pltpu.VMEM((4, rows, cols), f32),
            pltpu.VMEM(one, f32),
            pltpu.VMEM(one if coded else tiny, WIRE),
            pltpu.VMEM((2, zs, ins - 1, ins, rows, LANES), WIRE),
            pltpu.VMEM(two, f32),
            pltpu.VMEM(two if coded else tiny[1:], WIRE),
            pltpu.VMEM((2, zs, ins - 1, rows, LANES), WIRE),
            pltpu.VMEM((zs - 1, 2, rows, LANES), WIRE),
            pltpu.VMEM((2, rows, LANES), f32),
            pltpu.VMEM((zs - 1, 2, rows, LANES), WIRE),
            pltpu.SMEM(block_mask.shape, jnp.int32),
            dma((8,)),
            dma((zs, mps - 1)), dma((zs, mps - 1)),
            dma((2, zs, ins - 1)), dma((2, zs, ins - 1)),
            dma((2, zs, ins - 1)), dma((2, zs, ins - 1)),
            dma((zs - 1,)), dma((zs - 1,)),
            dma((zs - 1,)), dma((zs - 1,)),
            dma((2, zs, ins - 1)), dma((2, zs, ins - 1)),
            dma((2, zs, ins - 1)), dma((2, zs, ins - 1)),
            dma((zs, ins * ins - 1)), dma((zs, ins * ins - 1)),
        ],
        compiler_params=pltpu.CompilerParams(
            collective_id=0, has_side_effects=True, vmem_limit_bytes=48 * 1024 * 1024
        ),
    )(
        far(normed), far(key_grad), far(stale), worker_flag, far(block_mask),
        far(aggregate), far(master), far(moment_one), far(moment_two),
    )
    results = results[:4] + (results[4].reshape(depth, cols), results[5])
    results = pl.pallas_call(
        write_out,
        out_shape=tuple(pltpu.HBM(x.shape, x.dtype) for x in results),
        in_specs=[vmem] * 6,
        out_specs=(hbm,) * 6,
        scratch_shapes=[dma((6,))],
        compiler_params=pltpu.CompilerParams(vmem_limit_bytes=2 * 1024 * 1024),
    )(*results)
    return results[:5] + (results[5][None],)


def solution(mesh):
    placed = (
        P(("dp", "mp"), None),
        P("dp", "mp"),
        P("dp", None, "mp"),
        P("dp"),
        P("dp", None),
        P("dp", "mp"),
        P("dp", "mp"),
        P("dp", "mp"),
        P("dp", "mp"),
    )
    return jax.shard_map(
        functools.partial(on_device, mesh.shape["dp"], mesh.shape["mp"]),
        mesh=mesh,
        in_specs=placed,
        out_specs=(
            P("dp", "mp"),
            P("dp", "mp"),
            P("dp", "mp"),
            P("dp", "mp"),
            P(None, "mp"),
            P("dp", None, "mp"),
        ),
        check_vma=False,
    )
```
